16 devices in a mesh: dp: 2 (over y, z), ep: 8 (over x, core).
Axes of the slice: x: 4, y: 2, z: 1, core: 2. Of those that a mesh axis runs over, the one named last changes fastest.
The devices are a block of a 4x4x8 slice.
Arguments:
- tokens_a: bfloat16 [8192, 2048], P(('dp', 'ep')), parts along dimension 0
- experts_a: int32 [8192, 6], P(('dp', 'ep')), parts along dimension 0
- slots_a: int32 [8192, 6], P(('dp', 'ep')), parts along dimension 0
- gates_a: bfloat16 [8192, 6], P(('dp', 'ep')), parts along dimension 0
- tokens_b: bfloat16 [8192, 2048], P(('dp', 'ep')), parts along dimension 0
- experts_b: int32 [8192, 6], P(('dp', 'ep')), parts along dimension 0
- slots_b: int32 [8192, 6], P(('dp', 'ep')), parts along dimension 0
- gates_b: bfloat16 [8192, 6], P(('dp', 'ep')), parts along dimension 0
- attn_gain: bfloat16 [2048], replicated
- w_query: bfloat16 [2048, 16, 128], replicated
- w_key: bfloat16 [2048, 16, 128], replicated
- w_value: bfloat16 [2048, 16, 128], replicated
- w_out: bfloat16 [16, 128, 2048], replicated
- moe_gain: bfloat16 [2048], replicated
- w_gate: bfloat16 [64, 2048, 1408], P('ep')
- w_up: bfloat16 [64, 2048, 1408], P('ep')
- w_down: bfloat16 [64, 1408, 2048], P('ep')
Outputs:
- output 1: bfloat16 [8192, 2048], P(('dp', 'ep')), parts along dimension 0
- output 2: bfloat16 [8192, 2048], P(('dp', 'ep')), parts along dimension 0
There are 2 independent parts. The reference program is written for one: setup_inputs(seed, part) draws one part's arguments, and reference() takes and returns one part's arrays. A program takes and returns all parts, laid end to end along the dimension named above; an argument that names none is the same for every part.
All inputs are finite; a program needn't handle non-finite values.
Results may differ from the reference program's by a relative error of at most 0.0125727.
Values are sent between devices in bfloat16 or wider.
A program may use at most 768 MiB of HBM per device.

```python
import jax
import jax.numpy as jnp
from jax import lax

MODEL_DIM = 2048
FFN_DIM = 1408
EXPERTS = 64
TOP_K = 6
HEADS = 16
TOKENS = 512
GROUP = 8
SLOTS = 96

HEAD_DIM = MODEL_DIM // HEADS
ROWS = GROUP * TOKENS
NORM_EPS = 1e-6
MASK_VALUE = -1e30


def draw_routing(route_key):
    key_start, key_hot, key_pick = jax.random.split(route_key, 3)
    spacing = EXPERTS // TOP_K
    hot_span = max(1, EXPERTS // (4 * TOP_K))
    start_any = jax.random.randint(key_start, (ROWS,), 0, EXPERTS)
    start_hot = jax.random.randint(key_hot, (ROWS,), 0, hot_span)
    use_hot = jax.random.randint(key_pick, (ROWS,), 0, 2) == 1
    position = jnp.arange(ROWS) % TOKENS
    first_expert = jnp.where(use_hot, start_hot, start_any)
    first_expert = jnp.where(position <= SLOTS, 0, first_expert)
    choice = (first_expert[:, None] + spacing * jnp.arange(TOP_K)[None, :]) % EXPERTS
    choice = choice.astype(jnp.int32)

    def device_slots(dev_choice):
        flat_ids = dev_choice.reshape(-1)
        onehot = (flat_ids[:, None] == jnp.arange(EXPERTS)[None, :]).astype(jnp.int32)
        rank_pos = jnp.sum(jnp.cumsum(onehot, axis=0) * onehot, axis=1) - 1
        return jnp.where(rank_pos < SLOTS, rank_pos, -1).reshape(TOKENS, TOP_K)

    slot_ids = lax.map(device_slots, choice.reshape(GROUP, TOKENS, TOP_K))
    return choice, slot_ids.reshape(ROWS, TOP_K).astype(jnp.int32)


def setup_inputs(seed: int = 0, part: int = 0) -> dict:
    base_key = jax.random.key(seed)
    part_key = jax.random.fold_in(base_key, part)
    part_keys = jax.random.split(part_key, 6)
    shared_keys = jax.random.split(base_key, 9)
    scale_in = MODEL_DIM ** -0.5
    scale_ffn = FFN_DIM ** -0.5
    experts_a, slots_a = draw_routing(part_keys[1])
    experts_b, slots_b = draw_routing(part_keys[4])
    return {
        "tokens_a": jax.random.normal(part_keys[0], (ROWS, MODEL_DIM), jnp.float32).astype(jnp.bfloat16),
        "experts_a": experts_a,
        "slots_a": slots_a,
        "gates_a": jax.random.uniform(part_keys[2], (ROWS, TOP_K), jnp.float32, 0.5, 1.5).astype(jnp.bfloat16),
        "tokens_b": jax.random.normal(part_keys[3], (ROWS, MODEL_DIM), jnp.float32).astype(jnp.bfloat16),
        "experts_b": experts_b,
        "slots_b": slots_b,
        "gates_b": jax.random.uniform(part_keys[5], (ROWS, TOP_K), jnp.float32, 0.5, 1.5).astype(jnp.bfloat16),
        "attn_gain": (1.0 + 0.3 * jax.random.normal(shared_keys[0], (MODEL_DIM,), jnp.float32)).astype(jnp.bfloat16),
        "w_query": (1.5 * scale_in * jax.random.normal(shared_keys[1], (MODEL_DIM, HEADS, HEAD_DIM), jnp.float32)).astype(jnp.bfloat16),
        "w_key": (1.5 * scale_in * jax.random.normal(shared_keys[2], (MODEL_DIM, HEADS, HEAD_DIM), jnp.float32)).astype(jnp.bfloat16),
        "w_value": (scale_in * jax.random.normal(shared_keys[3], (MODEL_DIM, HEADS, HEAD_DIM), jnp.float32)).astype(jnp.bfloat16),
        "w_out": (scale_in * jax.random.normal(shared_keys[4], (HEADS, HEAD_DIM, MODEL_DIM), jnp.float32)).astype(jnp.bfloat16),
        "moe_gain": (1.0 + 0.3 * jax.random.normal(shared_keys[5], (MODEL_DIM,), jnp.float32)).astype(jnp.bfloat16),
        "w_gate": (scale_in * jax.random.normal(shared_keys[6], (EXPERTS, MODEL_DIM, FFN_DIM), jnp.float32)).astype(jnp.bfloat16),
        "w_up": (scale_in * jax.random.normal(shared_keys[7], (EXPERTS, MODEL_DIM, FFN_DIM), jnp.float32)).astype(jnp.bfloat16),
        "w_down": (scale_ffn * jax.random.normal(shared_keys[8], (EXPERTS, FFN_DIM, MODEL_DIM), jnp.float32)).astype(jnp.bfloat16),
    }


def rms_norm(rows, gain_vec):
    rows_f = rows.astype(jnp.float32)
    inv_rms = lax.rsqrt(jnp.mean(rows_f * rows_f, axis=-1, keepdims=True) + NORM_EPS)
    return (rows_f * inv_rms * gain_vec.astype(jnp.float32)).astype(jnp.bfloat16)


def attention_block(sequence, attn_gain, w_query, w_key, w_value, w_out):
    normed = rms_norm(sequence, attn_gain).astype(jnp.float32)
    query = jnp.einsum("td,dhe->the", normed, w_query.astype(jnp.float32)).astype(jnp.bfloat16)
    keys = jnp.einsum("td,dhe->the", normed, w_key.astype(jnp.float32)).astype(jnp.bfloat16)
    values = jnp.einsum("td,dhe->the", normed, w_value.astype(jnp.float32)).astype(jnp.bfloat16)
    scores = jnp.einsum("qhe,khe->hqk", query.astype(jnp.float32), keys.astype(jnp.float32)) * (HEAD_DIM ** -0.5)
    causal = jnp.arange(TOKENS)[:, None] >= jnp.arange(TOKENS)[None, :]
    scores = jnp.where(causal[None, :, :], scores, MASK_VALUE)
    attn_prob = jax.nn.softmax(scores, axis=-1).astype(jnp.bfloat16)
    context = jnp.einsum("hqk,khe->qhe", attn_prob.astype(jnp.float32), values.astype(jnp.float32)).astype(jnp.bfloat16)
    attn_out = jnp.einsum("qhe,hed->qd", context.astype(jnp.float32), w_out.astype(jnp.float32))
    return (sequence.astype(jnp.float32) + attn_out).astype(jnp.bfloat16)


def moe_layer(tokens, experts, slots, gates, attn_gain, w_query, w_key, w_value, w_out, moe_gain, w_gate, w_up, w_down):
    residual = lax.map(lambda sequence: attention_block(sequence, attn_gain, w_query, w_key, w_value, w_out), tokens.reshape(GROUP, TOKENS, MODEL_DIM))
    normed = rms_norm(residual, moe_gain).reshape(ROWS, MODEL_DIM)
    row_ids = jnp.arange(ROWS, dtype=jnp.int32)
    owner = row_ids // TOKENS
    buffer_rows = EXPERTS * GROUP * SLOTS
    dest_row = jnp.where(slots >= 0, experts * (GROUP * SLOTS) + owner[:, None] * SLOTS + slots, buffer_rows)
    token_of = jnp.broadcast_to(row_ids[:, None], (ROWS, TOP_K)).reshape(-1)
    source = jnp.full((buffer_rows,), ROWS, jnp.int32).at[dest_row.reshape(-1)].set(token_of, mode="drop")

    def expert_ffn(operands):
        expert_source, gate_w, up_w, down_w = operands
        rows_in = jnp.take(normed, expert_source, axis=0, mode="fill", fill_value=0)
        gate_act = jnp.dot(rows_in, gate_w, preferred_element_type=jnp.float32)
        up_act = jnp.dot(rows_in, up_w, preferred_element_type=jnp.float32)
        hidden = (jax.nn.silu(gate_act) * up_act).astype(jnp.bfloat16)
        return jnp.dot(hidden, down_w, preferred_element_type=jnp.float32).astype(jnp.bfloat16)

    expert_out = lax.map(expert_ffn, (source.reshape(EXPERTS, GROUP * SLOTS), w_gate, w_up, w_down)).reshape(buffer_rows, MODEL_DIM)

    def combine(operands):
        dev_resid, dev_dest, dev_gates = operands
        picked = jnp.take(expert_out, dev_dest, axis=0, mode="fill", fill_value=0).reshape(TOKENS, TOP_K, MODEL_DIM)
        mixed_sum = jnp.einsum("tk,tkd->td", dev_gates.astype(jnp.float32), picked.astype(jnp.float32))
        return (dev_resid.astype(jnp.float32) + mixed_sum).astype(jnp.bfloat16)

    mixed_rows = lax.map(combine, (residual, dest_row.reshape(GROUP, TOKENS * TOP_K), gates.reshape(GROUP, TOKENS, TOP_K)))
    return mixed_rows.reshape(ROWS, MODEL_DIM)


def reference(tokens_a, experts_a, slots_a, gates_a, tokens_b, experts_b, slots_b, gates_b, attn_gain, w_query, w_key, w_value, w_out, moe_gain, w_gate, w_up, w_down):
    out_a = moe_layer(tokens_a, experts_a, slots_a, gates_a, attn_gain, w_query, w_key, w_value, w_out, moe_gain, w_gate, w_up, w_down)
    out_b = moe_layer(tokens_b, experts_b, slots_b, gates_b, attn_gain, w_query, w_key, w_value, w_out, moe_gain, w_gate, w_up, w_down)
    return (out_a, out_b)
```

```python
import functools

import jax
import jax.numpy as jnp
from jax import lax
from jax.experimental import pallas as pl
from jax.experimental.pallas import tpu as pltpu
from jax.sharding import PartitionSpec as P

NORM_EPS = 1e-6
MASK_VALUE = -1e30
BLOCK = 16
TILE = 256
COUNT_ROW = 6
MOST_ROW = 7
BASE = 1024
VMEM_LIMIT = 62 * 1024 * 1024
F32 = jnp.float32
BF16 = jnp.bfloat16
I32 = jnp.int32


def rms_rows(rows_f, gain_f):
    inv_rms = lax.rsqrt(jnp.mean(rows_f * rows_f, axis=-1, keepdims=True) + NORM_EPS)
    return (rows_f * inv_rms * gain_f).astype(BF16)


def route_kernel(local_experts, top_k, experts_ref, slots_ref, table_ref, exact_ref):
    seq_len = experts_ref.shape[1]
    lanes = 128
    ids = experts_ref[0]
    slot = slots_ref[0]
    lane = lax.broadcasted_iota(I32, (seq_len, lanes), 1)
    hits = [jnp.where((ids[:, j : j + 1] == lane) & (slot[:, j : j + 1] >= 0), 1.0, 0.0) for j in range(top_k)]
    kept = functools.reduce(lambda a, b: a + b, hits)
    row = lax.broadcasted_iota(I32, (seq_len, seq_len), 0)
    col = lax.broadcasted_iota(I32, (seq_len, seq_len), 1)
    before = jnp.where(col < row, 1.0, 0.0).astype(BF16)
    rank = jnp.dot(before, kept.astype(BF16), preferred_element_type=F32)
    count8 = jnp.broadcast_to(jnp.sum(kept, axis=0, keepdims=True), (8, lanes))
    padded8 = ((count8.astype(I32) + (BLOCK - 1)) // BLOCK * BLOCK).astype(F32)
    erow = lax.broadcasted_iota(I32, (lanes, lanes), 0)
    ecol = lax.broadcasted_iota(I32, (lanes, lanes), 1)
    together = erow // local_experts == ecol // local_experts
    prefix = jnp.where((erow < ecol) & together, 1.0, 0.0).astype(BF16)
    exact_off = jnp.dot(count8.astype(BF16), prefix, preferred_element_type=F32)[0:1]
    aligned_off = jnp.dot(padded8.astype(BF16), prefix, preferred_element_type=F32)[0:1]
    total = jnp.dot(count8.astype(BF16), jnp.where(together, 1.0, 0.0).astype(BF16), preferred_element_type=F32)[0:1]
    device = (lax.broadcasted_iota(I32, (1, lanes), 1) // local_experts * BASE).astype(F32)
    aligned_row = rank + (aligned_off + device) + 1.0
    exact_row = rank + (exact_off + device) + 1.0
    aligned = jnp.zeros((seq_len, lanes), F32)
    exact = jnp.zeros((seq_len, lanes), F32)
    for j in range(top_k):
        aligned += jnp.where(lane == j, jnp.sum(hits[j] * aligned_row, axis=1, keepdims=True), 0.0)
        exact += jnp.where(lane == j, jnp.sum(hits[j] * exact_row, axis=1, keepdims=True), 0.0)
    table_ref[0] = (jnp.transpose(aligned, (1, 0))[:8]).astype(I32) - 1
    table_ref[0, COUNT_ROW : COUNT_ROW + 1, :lanes] = count8[:1].astype(I32)
    table_ref[0, MOST_ROW : MOST_ROW + 1, :lanes] = jnp.broadcast_to(
        jnp.max(total, axis=1, keepdims=True), (1, lanes)
    ).astype(I32)
    exact_ref[0] = exact[:, :8].astype(I32) - 1


def route(experts, slots, local_experts, group):
    batches, seq_len, top_k = experts.shape
    return pl.pallas_call(
        functools.partial(route_kernel, local_experts, top_k),
        grid=(batches,),
        in_specs=[pl.BlockSpec((1, seq_len, top_k), lambda b: (b, 0, 0))] * 2,
        out_specs=[
            pl.BlockSpec((1, 8, seq_len), lambda b: (b, 0, 0)),
            pl.BlockSpec((1, seq_len, 8), lambda b: (b, 0, 0)),
        ],
        out_shape=[
            jax.ShapeDtypeStruct((batches, 8, seq_len), I32),
            jax.ShapeDtypeStruct((batches, seq_len, 8), I32),
        ],
        compiler_params=pltpu.CompilerParams(vmem_limit_bytes=VMEM_LIMIT // 2),
        cost_estimate=pl.CostEstimate(flops=10**9, bytes_accessed=10**6, transcendentals=0),
        name="route",
    )(experts, slots)


def front_kernel(
    group, top_k, head_dim,
    xa_ref, xb_ref, q_ref, k_ref, v_ref, wo_ref, mgain_ref, table_ref,
    ha_ref, hb_ref, ua_ref, ub_ref, tables_ref, xs_ref,
    qkv, wo, xbuf, acc, hbuf, ubuf, codes, urows, xrows,
    q_sem, w_sem, x_sem, h_sem, u_sem, t_sem, load_sem, put_sem, send_sem, recv_sem, tsend_sem, trecv_sem,
):
    seq_len, model_dim = xbuf.shape
    half = seq_len // 2
    pairs = wo.shape[0]
    scale = head_dim**-0.5
    chips = group // 2
    me = lax.axis_index("ep")
    chip, core = me // 2, lax.rem(me, 2)
    mate = chip * 2 + 1 - core
    left = lax.rem(chip + chips - 1, chips) * 2 + core
    right = lax.rem(chip + 1, chips) * 2 + core
    far = lax.rem(chip + 2, chips) * 2 + core

    def weight_copy(p):
        return pltpu.make_async_copy(wo_ref.at[p], wo.at[p], w_sem.at[p])

    def qkv_copies(b):
        rows = pl.ds(b * seq_len, seq_len)
        return [
            pltpu.make_async_copy(src.at[:, rows], qkv.at[b, i], q_sem.at[b, i])
            for i, src in enumerate((q_ref, k_ref, v_ref))
        ]

    load_a = pltpu.make_async_copy(xa_ref, xbuf, x_sem.at[0])
    load_b = pltpu.make_async_copy(xb_ref, xbuf, x_sem.at[1])
    load_a.start()
    for c in qkv_copies(0):
        c.start()

    def start_weights(p, _):
        weight_copy(p).start()
        return 0

    lax.fori_loop(0, pairs, start_weights, 0)

    barrier = pltpu.get_barrier_semaphore()
    for d in range(1, group):
        pl.semaphore_signal(barrier, inc=1, device_id={"ep": lax.rem(me + d, group)}, device_id_type=pl.DeviceIdType.MESH)
    pl.semaphore_wait(barrier, group - 1)

    def table_copy(d, slot):
        return pltpu.make_async_remote_copy(
            src_ref=table_ref, dst_ref=tables_ref.at[slot], send_sem=tsend_sem.at[d], recv_sem=trecv_sem.at[d],
            device_id={"ep": lax.rem(me + d, group)}, device_id_type=pl.DeviceIdType.MESH,
        )

    own_table = pltpu.make_async_copy(table_ref, tables_ref.at[me], t_sem.at[0])
    own_table.start()
    for d in range(1, group):
        table_copy(d, me).start()

    part0, part1, both = pl.ds(0, half), pl.ds(half, half), pl.ds(0, seq_len)

    def u_copy(k, whose, rows, to):
        return pltpu.make_async_remote_copy(
            src_ref=ua_ref.at[whose, rows], dst_ref=ua_ref.at[whose, rows], send_sem=send_sem.at[k],
            recv_sem=recv_sem.at[k], device_id={"ep": to}, device_id_type=pl.DeviceIdType.MESH,
        )

    def mate_of(device):
        return device // 2 * 2 + 1 - lax.rem(device, 2)

    sends = [
        (me, part0, right), (me, part1, right), (me, part1, left), (me, part0, left),
        (left, part0, right), (right, part1, left), (me, both, mate),
        (left, part0, mate), (left, part1, mate), (right, part1, mate), (right, part0, mate),
        (far, part0, mate), (far, part1, mate),
    ]
    received = [
        left, left, right, right, far, far, mate,
        mate_of(left), mate_of(left), mate_of(right), mate_of(right), mate_of(far), mate_of(far),
    ]

    def send(k):
        u_copy(k, *sends[k]).start()

    def arrived(k):
        u_copy(k, received[k], sends[k][1], sends[k][2]).wait_recv()

    def attend_head(q, k, v, first_row):
        scores = lax.dot_general(q, k, (((1,), (1,)), ((), ())), preferred_element_type=F32) * scale
        rows = lax.broadcasted_iota(I32, scores.shape, 0) + first_row
        cols = lax.broadcasted_iota(I32, scores.shape, 1)
        scores = jnp.where(rows >= cols, scores, MASK_VALUE)
        top = jnp.max(scores, axis=-1, keepdims=True)
        e = jnp.exp(scores - top)
        prob = (e / jnp.sum(e, axis=-1, keepdims=True)).astype(BF16)
        return jnp.dot(prob, v, preferred_element_type=F32).astype(BF16)

    def begin():
        for r in range(0, seq_len, 128):
            acc[r : r + 128] = xbuf[r : r + 128].astype(F32)

    def head_pair(b, p):
        low, high = [], []
        for i in range(2):
            q, k, v = (qkv.at[b, n, 2 * p + i] for n in range(3))
            low.append(attend_head(q[:half], k[:half], v[:half], 0))
            high.append(attend_head(q[half:], k[...], v[...], half))
        w = wo[p]
        acc[:half] += jnp.dot(jnp.concatenate(low, axis=1), w, preferred_element_type=F32)
        acc[half:] += jnp.dot(jnp.concatenate(high, axis=1), w, preferred_element_type=F32)

    def finish():
        gain = mgain_ref[...].astype(F32)
        for r in range(0, seq_len, 128):
            h = acc[r : r + 128].astype(BF16)
            hbuf[r : r + 128] = h
            ubuf[r : r + 128] = rms_rows(h.astype(F32), gain)

    load_a.wait()
    begin()
    load_b.start()
    for c in qkv_copies(0):
        c.wait()
    for c in qkv_copies(1):
        c.start()

    def pair_a(p, _):
        weight_copy(p).wait()
        head_pair(0, p)
        return 0

    lax.fori_loop(0, pairs, pair_a, 0)
    finish()
    put_u = pltpu.make_async_copy(ubuf, ua_ref.at[me], u_sem.at[0])
    put_h = pltpu.make_async_copy(hbuf, ha_ref, h_sem.at[0])
    put_u.start()
    put_h.start()
    put_u.wait()
    for k in (0, 2, 6, 1, 3):
        send(k)

    load_b.wait()
    begin()
    for c in qkv_copies(1):
        c.wait()

    def pair_b(p, _):
        head_pair(1, p)

        @pl.when(p == pairs - 1)
        def _():
            arrived(0)
            send(4)
            send(7)
            arrived(2)
            send(5)
            send(9)

        return 0

    lax.fori_loop(0, pairs, pair_b, 0)
    put_h.wait()
    finish()
    put_ub = pltpu.make_async_copy(ubuf, ub_ref, u_sem.at[1])
    put_hb = pltpu.make_async_copy(hbuf, hb_ref, h_sem.at[1])
    put_ub.start()
    put_hb.start()

    own_table.wait()
    for d in range(1, group):
        table_copy(d, lax.rem(me + group - d, group)).wait_recv()
    load_codes = pltpu.make_async_copy(tables_ref.at[:, 0], codes, t_sem.at[1])
    load_codes.start()
    load_codes.wait()
    chunk = xrows.shape[1]
    chunks = xs_ref.shape[1] // chunk

    def select(source):
        load = pltpu.make_async_copy(ua_ref.at[source], urows, load_sem)
        load.start()
        load.wait()
        code = codes[source] - me * BASE

        def pick_chunk(i, _):
            row = lax.broadcasted_iota(I32, (chunk, seq_len), 0) + i * chunk
            pick = jnp.zeros((chunk, seq_len), F32)
            for j in range(top_k):
                pick = jnp.where(row == code[j : j + 1, :], 1.0, pick)
            slot = lax.rem(i, 2)
            put = pltpu.make_async_copy(
                xrows.at[slot], xs_ref.at[source, pl.ds(pl.multiple_of(i * chunk, chunk), chunk)], put_sem.at[slot]
            )

            @pl.when(i >= 2)
            def _():
                put.wait()

            xrows[slot] = jnp.dot(pick.astype(BF16), urows[...], preferred_element_type=F32).astype(BF16)
            put.start()
            return 0

        lax.fori_loop(0, chunks, pick_chunk, 0)
        for slot in range(2):
            pltpu.make_async_copy(xrows.at[slot], xs_ref.at[source, pl.ds(0, chunk)], put_sem.at[slot]).wait()

    select(me)
    arrived(6)
    select(mate)
    arrived(1)
    send(8)
    arrived(3)
    send(10)
    select(left)
    select(right)
    arrived(7)
    arrived(8)
    select(mate_of(left))
    arrived(9)
    arrived(10)
    select(mate_of(right))
    arrived(4)
    send(11)
    arrived(5)
    send(12)
    select(far)
    arrived(11)
    arrived(12)
    select(mate_of(far))

    for k in range(len(sends)):
        u_copy(k, *sends[k]).wait_send()
    for d in range(1, group):
        table_copy(d, me).wait_send()
    put_ub.wait()
    put_hb.wait()


def front(xa, xb, w_query, w_key, w_value, w_out, attn_gain, moe_gain, table, group, top_k, full_rows):
    seq_len, model_dim = xa.shape
    heads, head_dim = w_query.shape[1:]
    pairs = heads // 2
    wide = 2 * head_dim
    x = jnp.concatenate([xa, xb], axis=0)
    normed = rms_rows(x.astype(F32), attn_gain.astype(F32))
    q, k, v = (
        jnp.einsum("td,dhe->hte", normed, w, preferred_element_type=F32).astype(BF16) for w in (w_query, w_key, w_value)
    )
    wo = w_out.reshape(pairs, wide, model_dim)
    rows = jax.ShapeDtypeStruct((seq_len, model_dim), BF16)
    anywhere = pl.BlockSpec(memory_space=pl.ANY)
    vmem = pl.BlockSpec(memory_space=pltpu.VMEM)
    dma = pltpu.SemaphoreType.DMA
    chunk = 256
    return pl.pallas_call(
        functools.partial(front_kernel, group, top_k, head_dim),
        in_specs=[anywhere] * 6 + [vmem] * 2,
        out_specs=[anywhere] * 6,
        out_shape=[
            rows,
            rows,
            jax.ShapeDtypeStruct((group, seq_len, model_dim), BF16),
            rows,
            jax.ShapeDtypeStruct((group,) + table.shape, I32),
            jax.ShapeDtypeStruct((group, full_rows, model_dim), BF16),
        ],
        scratch_shapes=[
            pltpu.VMEM((2, 3, heads, seq_len, head_dim), BF16),
            pltpu.VMEM((pairs, wide, model_dim), BF16),
            pltpu.VMEM((seq_len, model_dim), BF16),
            pltpu.VMEM((seq_len, model_dim), F32),
            pltpu.VMEM((seq_len, model_dim), BF16),
            pltpu.VMEM((seq_len, model_dim), BF16),
            pltpu.VMEM((group,) + table.shape[1:], I32),
            pltpu.VMEM((seq_len, model_dim), BF16),
            pltpu.VMEM((2, chunk, model_dim), BF16),
            dma((2, 3)),
            dma((pairs,)),
            dma((2,)),
            dma((2,)),
            dma((2,)),
            dma((2,)),
            dma,
            dma((2,)),
            dma((13,)),
            dma((13,)),
            dma((group,)),
            dma((group,)),
        ],
        compiler_params=pltpu.CompilerParams(vmem_limit_bytes=VMEM_LIMIT, collective_id=0, has_side_effects=True),
        cost_estimate=pl.CostEstimate(
            flops=2 * (8 * seq_len * model_dim * model_dim + 4 * seq_len * seq_len * model_dim),
            bytes_accessed=2 * 4 * model_dim * model_dim,
            transcendentals=2 * heads * seq_len * seq_len,
        ),
        name="front",
    )(xa, xb, q, k, v, wo, moe_gain.reshape(1, -1), table)


def select_kernel(top_k, me_ref, code_ref, u_ref, out_ref):
    aligned_rows, seq_len = out_ref.shape[1], u_ref.shape[1]
    code = code_ref[0, 0] - me_ref[0] * BASE
    chunk = 160 if aligned_rows % 160 == 0 else 256
    for first in range(0, aligned_rows, chunk):
        row = lax.broadcasted_iota(I32, (chunk, seq_len), 0) + first
        pick = jnp.zeros((chunk, seq_len), F32)
        for j in range(top_k):
            pick = jnp.where(row == code[j : j + 1, :], 1.0, pick)
        out_ref[0, first : first + chunk] = jnp.dot(pick.astype(BF16), u_ref[0], preferred_element_type=F32).astype(BF16)


def select_rows(me, tables, batch, u_all, aligned_rows, top_k):
    group, seq_len, model_dim = u_all.shape
    return pl.pallas_call(
        functools.partial(select_kernel, top_k),
        grid_spec=pltpu.PrefetchScalarGridSpec(
            num_scalar_prefetch=1,
            grid=(group,),
            in_specs=[
                pl.BlockSpec((1, 1, 8, seq_len), lambda i, me: (i, batch, 0, 0)),
                pl.BlockSpec((1, seq_len, model_dim), lambda i, me: (i, 0, 0)),
            ],
            out_specs=pl.BlockSpec((1, aligned_rows, model_dim), lambda i, me: (i, 0, 0)),
        ),
        out_shape=jax.ShapeDtypeStruct((group, aligned_rows, model_dim), BF16),
        compiler_params=pltpu.CompilerParams(vmem_limit_bytes=VMEM_LIMIT),
        cost_estimate=pl.CostEstimate(
            flops=2 * group * aligned_rows * seq_len * model_dim,
            bytes_accessed=2 * group * (aligned_rows + seq_len) * model_dim,
            transcendentals=0,
        ),
        name="select",
    )(me, tables, u_all)


def expert_kernel(me_ref, count_ref, x_in, gate_ref, up_ref, down_ref, x_out, buf, blocks_ref, offset_ref, in_sem, out_sem):
    step = pl.program_id(0)
    steps = pl.num_programs(0)
    places = x_in.shape[0]

    def each_block(expert, slot, fn):
        def per_place(place, filled):
            n = blocks_ref[place, expert]
            first = offset_ref[place, expert]

            def per_block(b, _):
                rows = pl.ds(pl.multiple_of(first + b * BLOCK, BLOCK), BLOCK)
                held = pl.ds(pl.multiple_of((filled + b) * BLOCK, BLOCK), BLOCK)
                fn(place, rows, buf.at[slot, held])
                return 0

            lax.fori_loop(0, n, per_block, 0)
            return filled + n

        return lax.fori_loop(0, places, per_place, jnp.int32(0))

    def fetch(place, rows, held, slot):
        pltpu.make_async_copy(x_in.at[place, rows], held, in_sem.at[slot]).start()

    def put(place, rows, held, slot):
        pltpu.make_async_copy(held, x_out.at[place, rows], out_sem.at[slot]).start()

    def fetched(place, rows, held, slot):
        pltpu.make_async_copy(x_in.at[place, rows], held, in_sem.at[slot]).wait()

    def gone(place, rows, held, slot):
        pltpu.make_async_copy(held, x_out.at[place, rows], out_sem.at[slot]).wait()

    def over(expert, fn):
        slot = lax.rem(expert, 3)
        return each_block(expert, slot, functools.partial(fn, slot=slot))

    @pl.when(step == 0)
    def _():
        def plan(place, _):
            def one(e, filled):
                n = (count_ref[place, me_ref[0] * steps + e] + (BLOCK - 1)) // BLOCK
                blocks_ref[place, e] = n
                offset_ref[place, e] = filled * BLOCK
                return filled + n

            lax.fori_loop(0, steps, one, jnp.int32(0))
            return 0

        lax.fori_loop(0, places, plan, 0)
        over(step, fetch)

    @pl.when(step >= 2)
    def _():
        over(step - 2, gone)

    @pl.when(step + 1 < steps)
    def _():
        over(step + 1, fetch)

    filled = over(step, fetched)
    slot = lax.rem(step, 3)

    def tile(i, _):
        rows = pl.ds(pl.multiple_of(i * TILE, TILE), TILE)
        x = buf[slot, rows]
        gate = jnp.dot(x, gate_ref[0], preferred_element_type=F32)
        up = jnp.dot(x, up_ref[0], preferred_element_type=F32)
        hidden = (gate * jax.nn.sigmoid(gate) * up).astype(BF16)
        buf[slot, rows] = jnp.dot(hidden, down_ref[0], preferred_element_type=F32).astype(BF16)
        return 0

    lax.fori_loop(0, (filled * BLOCK + TILE - 1) // TILE, tile, 0)
    over(step, put)

    @pl.when(step + 1 == steps)
    def _():
        over(step - 1, gone)
        over(step, gone)


def expert_ffn(me, counts, x, w_gate, w_up, w_down, capacity):
    places, aligned_rows, model_dim = x.shape
    experts, _, hidden_dim = w_gate.shape
    held = -(-places * capacity // TILE) * TILE
    weight_in = pl.BlockSpec((1, model_dim, hidden_dim), lambda e, b, o: (e, 0, 0))
    return pl.pallas_call(
        expert_kernel,
        grid_spec=pltpu.PrefetchScalarGridSpec(
            num_scalar_prefetch=2,
            grid=(experts,),
            in_specs=[
                pl.BlockSpec(memory_space=pl.ANY),
                weight_in,
                weight_in,
                pl.BlockSpec((1, hidden_dim, model_dim), lambda e, b, o: (e, 0, 0)),
            ],
            out_specs=pl.BlockSpec(memory_space=pl.ANY),
            scratch_shapes=[
                pltpu.VMEM((3, held, model_dim), BF16),
                pltpu.SMEM((places, experts), I32),
                pltpu.SMEM((places, experts), I32),
                pltpu.SemaphoreType.DMA((3,)),
                pltpu.SemaphoreType.DMA((3,)),
            ],
        ),
        out_shape=jax.ShapeDtypeStruct(x.shape, BF16),
        input_output_aliases={2: 0},
        compiler_params=pltpu.CompilerParams(vmem_limit_bytes=VMEM_LIMIT),
        cost_estimate=pl.CostEstimate(
            flops=6 * 3072 * model_dim * hidden_dim,
            bytes_accessed=6 * experts * model_dim * hidden_dim,
            transcendentals=0,
        ),
        name="experts",
    )(me, counts, x, w_gate, w_up, w_down)


def pack_kernel(local_experts, me_ref, count_ref, x_ref, out_ref):
    rows_out, aligned_rows = out_ref.shape[1], x_ref.shape[1]
    place = pl.program_id(0)
    chunk = 176 if rows_out % 176 == 0 else 256
    for first in range(0, rows_out, chunk):
        row = lax.broadcasted_iota(I32, (chunk, 1), 0) + first
        source = jnp.full((chunk, 1), -1, I32)
        off, aligned_off = jnp.int32(0), jnp.int32(0)
        for e in range(local_experts):
            n = count_ref[place, me_ref[0] * local_experts + e]
            inside = (row >= off) & (row < off + n)
            source = jnp.where(inside, row + (aligned_off - off), source)
            off = off + n
            aligned_off = aligned_off + (n + (BLOCK - 1)) // BLOCK * BLOCK
        col = lax.broadcasted_iota(I32, (chunk, aligned_rows), 1)
        pick = jnp.where(col == source, 1.0, 0.0).astype(BF16)
        out_ref[0, first : first + chunk] = jnp.dot(pick, x_ref[0], preferred_element_type=F32).astype(BF16)


def pack_rows(me, counts, x, local_experts, aligned_rows, rows_out):
    places, _, model_dim = x.shape
    return pl.pallas_call(
        functools.partial(pack_kernel, local_experts),
        grid_spec=pltpu.PrefetchScalarGridSpec(
            num_scalar_prefetch=2,
            grid=(places,),
            in_specs=[pl.BlockSpec((1, aligned_rows, model_dim), lambda i, m, c: (i, 0, 0))],
            out_specs=pl.BlockSpec((1, rows_out, model_dim), lambda i, m, c: (i, 0, 0)),
        ),
        out_shape=jax.ShapeDtypeStruct((places, rows_out, model_dim), BF16),
        compiler_params=pltpu.CompilerParams(vmem_limit_bytes=VMEM_LIMIT),
        cost_estimate=pl.CostEstimate(
            flops=2 * places * aligned_rows * rows_out * model_dim,
            bytes_accessed=2 * places * (aligned_rows + rows_out) * model_dim,
            transcendentals=0,
        ),
        name="pack",
    )(me, counts, x)


def combine_kernel(top_k, code_ref, gates_ref, recv_ref, h_ref, out_ref, acc_ref):
    step = pl.program_id(0)
    rows = recv_ref.shape[0]

    @pl.when(step == 0)
    def _():
        acc_ref[...] = h_ref[...].astype(F32)

    code = code_ref[...]
    gates = gates_ref[...]
    col = lax.broadcasted_iota(I32, (code.shape[0], rows), 1) + step * rows
    mix = jnp.zeros(col.shape, F32)
    for j in range(top_k):
        mix = jnp.where(col == code[:, j : j + 1], gates[:, j : j + 1], mix)
    acc_ref[...] += jnp.dot(mix.astype(BF16), recv_ref[...], preferred_element_type=F32)

    @pl.when(step == pl.num_programs(0) - 1)
    def _():
        out_ref[...] = acc_ref[...].astype(BF16)


def combine(residual, recv, code, gates):
    seq_len, model_dim = residual.shape
    group, rows, _ = recv.shape
    top_k = gates.shape[1]
    column = jnp.where(code >= 0, code // BASE * rows + code % BASE, -1)
    gates_f = jnp.pad(gates.astype(F32), ((0, 0), (0, 8 - top_k)))
    rows_step = 256
    whole = lambda r, c: pl.BlockSpec((r, c), lambda i: (0, 0))
    return pl.pallas_call(
        functools.partial(combine_kernel, top_k),
        grid=(group * rows // rows_step,),
        in_specs=[
            whole(seq_len, 8),
            whole(seq_len, 8),
            pl.BlockSpec((rows_step, model_dim), lambda i: (i, 0)),
            whole(seq_len, model_dim),
        ],
        out_specs=whole(seq_len, model_dim),
        out_shape=jax.ShapeDtypeStruct((seq_len, model_dim), BF16),
        scratch_shapes=[pltpu.VMEM((seq_len, model_dim), F32)],
        compiler_params=pltpu.CompilerParams(vmem_limit_bytes=VMEM_LIMIT),
        cost_estimate=pl.CostEstimate(
            flops=2 * seq_len * group * rows * model_dim,
            bytes_accessed=2 * (group * rows + 2 * seq_len) * model_dim,
            transcendentals=0,
        ),
        name="combine",
    )(column, gates_f, recv.reshape(group * rows, model_dim), residual)


def capacity_of(seq_len, top_k, experts_total):
    return 8 * max(1, (seq_len * top_k) // (4 * experts_total))


def solution(mesh):
    group = mesh.shape["ep"]
    row_spec = P(("dp", "ep"), None)
    full_spec = P(None, None, None)
    gain_spec = P(None)
    expert_spec = P("ep", None, None)
    in_specs = (row_spec,) * 8 + (gain_spec, full_spec, full_spec, full_spec, full_spec, gain_spec) + (expert_spec,) * 3

    def device_fn(
        tokens_a, experts_a, slots_a, gates_a, tokens_b, experts_b, slots_b, gates_b,
        attn_gain, w_query, w_key, w_value, w_out, moe_gain, w_gate, w_up, w_down,
    ):
        seq_len, model_dim = tokens_a.shape
        local_experts = w_gate.shape[0]
        capacity = capacity_of(seq_len, experts_a.shape[1], local_experts * group)
        full_rows = local_experts * capacity
        me = lax.axis_index("ep").astype(I32)

        top_k = experts_a.shape[1]
        me1 = me.reshape(1)
        table, exact = route(jnp.stack([experts_a, experts_b]), jnp.stack([slots_a, slots_b]), local_experts, group)
        h_a, h_b, _, u_b, tables, x_a = front(
            tokens_a, tokens_b, w_query, w_key, w_value, w_out, attn_gain, moe_gain, table, group, top_k, full_rows
        )
        counts = tables[:, :, COUNT_ROW, : local_experts * group]
        largest = jnp.max(tables[:, :, MOST_ROW, 0])

        def moe(rows_out, aligned_rows, operands):
            x_a, u_b, h_a, h_b, tables, counts = operands

            def experts_side(b, x):
                o = expert_ffn(me1, counts[:, b], x, w_gate, w_up, w_down, capacity)
                packed = pack_rows(me1, counts[:, b], o, local_experts, aligned_rows, rows_out)
                return lax.all_to_all(packed, "ep", 0, 0, tiled=True)

            u_all = lax.all_gather(u_b, "ep", axis=0, tiled=False)
            back_a = experts_side(0, x_a)
            back_b = experts_side(1, select_rows(me1, tables, 1, u_all, aligned_rows, top_k))
            return combine(h_a, back_a, exact[0], gates_a), combine(h_b, back_b, exact[1], gates_b)

        sizes = [r for r in (352,) if r < full_rows] + [full_rows]
        branches = []
        for r in sizes:
            aligned_rows = min(full_rows, -(-(r + local_experts * (BLOCK - 1)) // 160) * 160)
            branches.append(functools.partial(moe, r, aligned_rows))
        which = jnp.int32(0)
        for r in sizes[:-1]:
            which = which + (largest > r).astype(I32)
        return lax.switch(which, branches, (x_a, u_b, h_a, h_b, tables, counts))

    return jax.shard_map(device_fn, mesh=mesh, in_specs=in_specs, out_specs=(row_spec, row_spec), check_vma=False)
```

```python
import functools

import jax
import jax.numpy as jnp
from jax import lax
from jax.experimental import pallas as pl
from jax.experimental.pallas import tpu as pltpu
from jax.sharding import PartitionSpec as P

NORM_EPS = 1e-6
MASK_VALUE = -1e30
BLOCK = 16
TILE = 256
COUNT_ROW = 6
MOST_ROW = 7
BASE = 1024
VMEM_LIMIT = 65011712
F32 = jnp.float32
BF16 = jnp.bfloat16
I32 = jnp.int32
NONE = 0
SMALL = pl.CostEstimate(flops=1000000, bytes_accessed=1000000, transcendentals=NONE)


def at_origin(i):
    return (0, 0)


def by_place(i, *_):
    return (i, 0, 0)


def pieces(last, first=0):
    return [slice(r, r + 128) for r in range(first, last, 128)]


def repeat(times, body):
    lax.fori_loop(0, times, body, 0)


def row_ids(shape):
    return lax.broadcasted_iota(I32, shape, 0)


def col_ids(shape):
    return lax.broadcasted_iota(I32, shape, 1)


def rms_rows(rows_f, gain_f):
    inv_rms = lax.rsqrt(jnp.mean(rows_f * rows_f, axis=-1, keepdims=True) + NORM_EPS)
    return (rows_f * inv_rms * gain_f).astype(BF16)


def route_kernel(local_experts, top_k, experts_ref, slots_ref, table_ref, exact_ref):
    seq_len = experts_ref.shape[1]
    lanes = 128
    ids = experts_ref[0]
    slot = slots_ref[0]
    lane = col_ids((seq_len, lanes))
    hits = [jnp.where((ids[:, j : j + 1] == lane) & (slot[:, j : j + 1] >= 0), 1.0, 0.0) for j in range(top_k)]
    kept = functools.reduce(lambda a, b: a + b, hits)
    row = row_ids((seq_len, seq_len))
    col = col_ids((seq_len, seq_len))
    before = jnp.where(col < row, 1.0, 0.0).astype(BF16)
    rank = jnp.dot(before, kept.astype(BF16), preferred_element_type=F32)
    count8 = jnp.broadcast_to(jnp.sum(kept, axis=0, keepdims=True), (8, lanes))
    padded8 = ((count8.astype(I32) + (BLOCK - 1)) // BLOCK * BLOCK).astype(F32)
    erow = row_ids((lanes, lanes))
    ecol = col_ids((lanes, lanes))
    together = erow // local_experts == ecol // local_experts
    prefix = jnp.where((erow < ecol) & together, 1.0, 0.0).astype(BF16)
    exact_off = jnp.dot(count8.astype(BF16), prefix, preferred_element_type=F32)[0:1]
    aligned_off = jnp.dot(padded8.astype(BF16), prefix, preferred_element_type=F32)[0:1]
    total = jnp.dot(count8.astype(BF16), jnp.where(together, 1.0, 0.0).astype(BF16), preferred_element_type=F32)[0:1]
    device = (col_ids((1, lanes)) // local_experts * BASE).astype(F32)
    aligned_row = rank + (aligned_off + device) + 1.0
    exact_row = rank + (exact_off + device) + 1.0
    aligned = jnp.zeros((seq_len, lanes), F32)
    exact = jnp.zeros((seq_len, lanes), F32)
    for j in range(top_k):
        aligned += jnp.where(lane == j, jnp.sum(hits[j] * aligned_row, axis=1, keepdims=True), 0.0)
        exact += jnp.where(lane == j, jnp.sum(hits[j] * exact_row, axis=1, keepdims=True), 0.0)
    table_ref[0] = (jnp.transpose(aligned, (1, 0))[:8]).astype(I32) - 1
    table_ref[0, COUNT_ROW : COUNT_ROW + 1, :lanes] = count8[:1].astype(I32)
    table_ref[0, MOST_ROW : MOST_ROW + 1, :lanes] = jnp.broadcast_to(
        jnp.max(total, axis=1, keepdims=True), (1, lanes)
    ).astype(I32)
    exact_ref[0] = exact[:, :8].astype(I32) - 1


def route(experts, slots, local_experts, group):
    batches, seq_len, top_k = experts.shape
    return pl.pallas_call(
        functools.partial(route_kernel, local_experts, top_k),
        grid=(batches,),
        in_specs=[pl.BlockSpec((1, seq_len, top_k), by_place)] * 2,
        out_specs=[
            pl.BlockSpec((1, 8, seq_len), by_place),
            pl.BlockSpec((1, seq_len, 8), by_place),
        ],
        out_shape=[
            jax.ShapeDtypeStruct((batches, 8, seq_len), I32),
            jax.ShapeDtypeStruct((batches, seq_len, 8), I32),
        ],
        compiler_params=pltpu.CompilerParams(vmem_limit_bytes=VMEM_LIMIT // 2),
        cost_estimate=SMALL,
        name="route",
    )(experts, slots)


def front_kernel(
    group, top_k, head_dim,
    xa_ref, xb_ref, q_ref, k_ref, v_ref, wo_ref, mgain_ref, table_ref,
    ha_ref, hb_ref, ua_ref, ub_ref, tables_ref, xs_ref,
    qkv, wo, xbuf, acc, hbuf, ubuf, codes, urows, xrows, picks,
    q_sem, w_sem, x_sem, h_sem, u_sem, t_sem, load_sem, put_sem, send_sem, recv_sem, tsend_sem, trecv_sem,
):
    seq_len, model_dim = xbuf.shape
    half = seq_len // 2
    pairs = wo.shape[0]
    scale = head_dim**-0.5
    chips = group // 2
    me = lax.axis_index("ep")
    chip, core = me // 2, lax.rem(me, 2)
    mate = chip * 2 + 1 - core
    left = lax.rem(chip + chips - 1, chips) * 2 + core
    right = lax.rem(chip + 1, chips) * 2 + core
    far = lax.rem(chip + 2, chips) * 2 + core

    def weight_copy(p):
        return pltpu.make_async_copy(wo_ref.at[p], wo.at[p], w_sem.at[p])

    def qkv_copies(b):
        rows = pl.ds(b * seq_len, seq_len)
        return [
            pltpu.make_async_copy(src.at[:, rows], qkv.at[b, i], q_sem.at[b, i])
            for i, src in enumerate((q_ref, k_ref, v_ref))
        ]

    load_a = pltpu.make_async_copy(xa_ref, xbuf, x_sem.at[0])
    load_b = pltpu.make_async_copy(xb_ref, xbuf, x_sem.at[1])
    load_a.start()
    for c in qkv_copies(0):
        c.start()

    def start_weights(p, _):
        weight_copy(p).start()
        return 0

    repeat(pairs, start_weights)

    barrier = pltpu.get_barrier_semaphore()
    for d in range(1, group):
        pl.semaphore_signal(barrier, device_id={"ep": lax.rem(me + d, group)}, device_id_type=pl.DeviceIdType.MESH)
    pl.semaphore_wait(barrier, group - 1)

    def table_copy(d, slot):
        return pltpu.make_async_remote_copy(
            src_ref=table_ref, dst_ref=tables_ref.at[slot], send_sem=tsend_sem.at[d], recv_sem=trecv_sem.at[d],
            device_id={"ep": lax.rem(me + d, group)}, device_id_type=pl.DeviceIdType.MESH,
        )

    own_table = pltpu.make_async_copy(table_ref, tables_ref.at[me], t_sem.at[0])
    own_table.start()
    for d in range(1, group):
        table_copy(d, me).start()

    part0, part1, both = pl.ds(0, half), pl.ds(half, half), pl.ds(0, seq_len)

    def u_copy(k, whose, rows, to):
        return pltpu.make_async_remote_copy(
            src_ref=ua_ref.at[whose, rows], dst_ref=ua_ref.at[whose, rows], send_sem=send_sem.at[k],
            recv_sem=recv_sem.at[k], device_id={"ep": to}, device_id_type=pl.DeviceIdType.MESH,
        )

    def mate_of(device):
        return device // 2 * 2 + 1 - lax.rem(device, 2)

    sends = [
        (me, part0, right), (me, part1, right), (me, part1, left), (me, part0, left),
        (left, part0, right), (right, part1, left), (me, both, mate),
        (left, part0, mate), (left, part1, mate), (right, part1, mate), (right, part0, mate),
        (far, part0, mate), (far, part1, mate),
    ]
    received = [
        left, left, right, right, far, far, mate,
        mate_of(left), mate_of(left), mate_of(right), mate_of(right), mate_of(far), mate_of(far),
    ]

    def send(k):
        u_copy(k, *sends[k]).start()

    def arrived(k):
        u_copy(k, received[k], sends[k][1], sends[k][2]).wait_recv()

    def attend_head(q, k, v, first_row):
        scores = lax.dot_general(q, k, (((1,), (1,)), ((), ())), preferred_element_type=F32) * scale
        rows = row_ids(scores.shape) + first_row
        cols = col_ids(scores.shape)
        scores = jnp.where(rows >= cols, scores, MASK_VALUE)
        top = jnp.max(scores, axis=-1, keepdims=True)
        e = jnp.exp(scores - top)
        prob = (e * (1.0 / jnp.sum(e, axis=-1, keepdims=True))).astype(BF16)
        return jnp.dot(prob, v, preferred_element_type=F32).astype(BF16)

    def begin():
        for piece in pieces(seq_len):
            acc[piece] = xbuf[piece].astype(F32)

    def low_half(b, p, n_pairs=1):
        outs = []
        for j in range(n_pairs):
            heads = []
            for i in range(2):
                q, k, v = (qkv.at[b, n, 2 * (p + j) + i] for n in range(3))
                heads.append(attend_head(q[:half], k[:half], v[:half], 0))
            outs.append(jnp.dot(jnp.concatenate(heads, axis=1), wo[p + j], preferred_element_type=F32))
        acc[:half] += functools.reduce(lambda x, y: x + y, outs)

    def high_half(b, p, n_pairs=1):
        outs = []
        for j in range(n_pairs):
            heads = []
            for i in range(2):
                q, k, v = (qkv.at[b, n, 2 * (p + j) + i] for n in range(3))
                heads.append(attend_head(q[half:], k[...], v[...], half))
            outs.append(jnp.dot(jnp.concatenate(heads, axis=1), wo[p + j], preferred_element_type=F32))
        acc[half:] += functools.reduce(lambda x, y: x + y, outs)

    def finish(first, last):
        gain = mgain_ref[...].astype(F32)
        for piece in pieces(last, first):
            h = acc[piece].astype(BF16)
            hbuf[piece] = h
            ubuf[piece] = rms_rows(h.astype(F32), gain)

    load_a.wait()
    begin()
    load_b.start()
    for c in qkv_copies(0):
        c.wait()
    for c in qkv_copies(1):
        c.start()

    def low_a(p, _):
        weight_copy(2 * p).wait()
        weight_copy(2 * p + 1).wait()
        low_half(0, 2 * p, 2)
        return 0

    def high_a(p, _):
        high_half(0, 2 * p, 2)
        return 0

    def put_part(part, i):
        return pltpu.make_async_copy(ubuf.at[part], ua_ref.at[me, part], u_sem.at[i])

    repeat(pairs // 2, low_a)
    finish(0, half)
    put_part(part0, 0).start()
    put_part(part0, 0).wait()
    send(0)
    send(3)
    repeat(pairs // 2, high_a)
    finish(half, seq_len)
    put_part(part1, 2).start()
    put_part(part1, 2).wait()
    send(2)
    send(1)
    send(6)
    put_h = pltpu.make_async_copy(hbuf, ha_ref, h_sem.at[0])
    put_h.start()

    load_b.wait()
    begin()
    for c in qkv_copies(1):
        c.wait()

    def pair_b(p, _):
        low_half(1, p)
        high_half(1, p)

        @pl.when(p == pairs - 1)
        def _():
            arrived(0)
            send(4)
            send(7)
            arrived(2)
            send(5)
            send(9)

        return 0

    repeat(pairs, pair_b)
    put_h.wait()
    finish(0, seq_len)
    put_ub = pltpu.make_async_copy(ubuf, ub_ref, u_sem.at[1])
    put_hb = pltpu.make_async_copy(hbuf, hb_ref, h_sem.at[1])
    put_ub.start()
    put_hb.start()

    own_table.wait()
    for d in range(1, group):
        table_copy(d, lax.rem(me + group - d, group)).wait_recv()
    load_codes = pltpu.make_async_copy(tables_ref.at[:, 0], codes, t_sem.at[1])
    load_codes.start()
    load_codes.wait()
    chunks, chunk = xrows.shape[1:3]

    def load(source, slot):
        return pltpu.make_async_copy(ua_ref.at[source], urows.at[slot], load_sem.at[slot])

    def build(source, slot):
        code = codes[source] - me * BASE

        def chunk_of(i, _):
            row = row_ids((chunk, seq_len)) + i * chunk
            pick = jnp.zeros((chunk, seq_len), F32)
            for j in range(top_k):
                pick = jnp.where(row == code[j : j + 1, :], 1.0, pick)
            picks[slot, pl.ds(pl.multiple_of(i * chunk, chunk), chunk)] = pick.astype(BF16)
            return 0

        repeat(chunks, chunk_of)

    def put_rows(source, i, slot):
        rows = pl.ds(pl.multiple_of(i * chunk, chunk), chunk)
        return pltpu.make_async_copy(xrows.at[slot, i], xs_ref.at[source, rows], put_sem.at[slot, i])

    def select(source, slot, first, last):
        def chunk_of(i, _):
            pick = picks[slot, pl.ds(pl.multiple_of(i * chunk, chunk), chunk)]
            xrows[slot, i] = jnp.dot(pick, urows[slot], preferred_element_type=F32).astype(BF16)
            put_rows(source, i, slot).start()
            return 0

        lax.fori_loop(first, last, chunk_of, 0)

    def put_done(source, slot):
        for i in range(chunks):
            put_rows(source, i, slot).wait()

    def source_at(i):
        return lax.rem(chip + lax.rem(i // 2 * 3, 5), chips) * 2 + lax.rem(core + i, 2)

    def near(i, _):
        slot = lax.rem(i, 2)
        source = source_at(i)

        @pl.when(i == 1)
        def _():
            arrived(6)

        @pl.when(i == 2)
        def _():
            arrived(1)
            send(8)
            arrived(3)
            send(10)

        @pl.when(i == 3)
        def _():
            arrived(7)
            arrived(8)

        @pl.when(i == 5)
        def _():
            arrived(9)
            arrived(10)

        load(source, slot).start()
        build(source, slot)

        @pl.when(i >= 2)
        def _():
            put_done(source_at(i - 2), slot)

        load(source, slot).wait()
        select(source, slot, 0, chunks)
        return 0

    repeat(6, near)
    build(far, 0)
    build(mate_of(far), 1)
    put_done(source_at(4), 0)
    put_done(source_at(5), 1)
    arrived(4)
    send(11)
    arrived(5)
    send(12)
    load(far, 0).start()
    load(far, 0).wait()
    select(far, 0, 0, 1)
    arrived(11)
    arrived(12)
    load(mate_of(far), 1).start()
    select(far, 0, 1, chunks)
    load(mate_of(far), 1).wait()
    select(mate_of(far), 1, 0, chunks)
    put_done(far, 0)
    put_done(mate_of(far), 1)

    for k in range(len(sends)):
        u_copy(k, *sends[k]).wait_send()
    for d in range(1, group):
        table_copy(d, me).wait_send()
    put_ub.wait()
    put_hb.wait()


def front(xa, xb, w_query, w_key, w_value, w_out, attn_gain, moe_gain, table, group, top_k, full_rows):
    seq_len, model_dim = xa.shape
    heads, head_dim = w_query.shape[1:]
    pairs = heads // 2
    wide = 2 * head_dim
    x = jnp.concatenate([xa, xb], axis=0)
    normed = rms_rows(x.astype(F32), attn_gain.astype(F32))
    q, k, v = (
        jnp.einsum("td,dhe->hte", normed, w, preferred_element_type=F32).astype(BF16) for w in (w_query, w_key, w_value)
    )
    wo = w_out.reshape(pairs, wide, model_dim)
    rows = jax.ShapeDtypeStruct((seq_len, model_dim), BF16)
    anywhere = pl.BlockSpec(memory_space=pl.ANY)
    vmem = pl.BlockSpec(memory_space=pltpu.VMEM)
    dma = pltpu.SemaphoreType.DMA
    pair = dma((2,))
    chunk = 256
    return pl.pallas_call(
        functools.partial(front_kernel, group, top_k, head_dim),
        in_specs=[anywhere] * 6 + [vmem] * 2,
        out_specs=[anywhere] * 6,
        out_shape=[
            rows,
            rows,
            jax.ShapeDtypeStruct((group, seq_len, model_dim), BF16),
            rows,
            jax.ShapeDtypeStruct((group,) + table.shape, I32),
            jax.ShapeDtypeStruct((group, full_rows, model_dim), BF16),
        ],
        scratch_shapes=[
            pltpu.VMEM((2, 3, heads, seq_len, head_dim), BF16),
            pltpu.VMEM((pairs, wide, model_dim), BF16),
            pltpu.VMEM((seq_len, model_dim), BF16),
            pltpu.VMEM((seq_len, model_dim), F32),
            pltpu.VMEM((seq_len, model_dim), BF16),
            pltpu.VMEM((seq_len, model_dim), BF16),
            pltpu.VMEM((group,) + table.shape[1:], I32),
            pltpu.VMEM((2, seq_len, model_dim), BF16),
            pltpu.VMEM((2, full_rows // chunk, chunk, model_dim), BF16),
            pltpu.VMEM((2, full_rows, seq_len), BF16),
            dma((2, 3)),
            dma((pairs,)),
            pair,
            pair,
            dma((3,)),
            pair,
            pair,
            dma((2, full_rows // chunk)),
            dma((13,)),
            dma((13,)),
            dma((group,)),
            dma((group,)),
        ],
        compiler_params=pltpu.CompilerParams(vmem_limit_bytes=VMEM_LIMIT, collective_id=0, has_side_effects=True),
        cost_estimate=pl.CostEstimate(
            flops=2 * (8 * seq_len * model_dim * model_dim + 4 * seq_len * seq_len * model_dim),
            bytes_accessed=2 * 4 * model_dim * model_dim,
            transcendentals=2 * heads * seq_len * seq_len,
        ),
        name="front",
    )(xa, xb, q, k, v, wo, moe_gain.reshape(1, -1), table)


def select_kernel(top_k, me_ref, code_ref, u_ref, out_ref):
    aligned_rows, seq_len = out_ref.shape[1], u_ref.shape[1]
    code = code_ref[0] - me_ref[0] * BASE
    chunk = aligned_rows if aligned_rows <= 512 else 256
    for first in range(0, aligned_rows, chunk):
        row = row_ids((chunk, seq_len)) + first
        pick = jnp.zeros((chunk, seq_len), F32)
        for j in range(top_k):
            pick = jnp.where(row == code[j : j + 1, :], 1.0, pick)
        out_ref[0, first : first + chunk] = jnp.dot(pick.astype(BF16), u_ref[0], preferred_element_type=F32).astype(BF16)


def select_rows(me, codes, u_all, aligned_rows, top_k):
    group, seq_len, model_dim = u_all.shape
    return pl.pallas_call(
        functools.partial(select_kernel, top_k),
        grid_spec=pltpu.PrefetchScalarGridSpec(
            num_scalar_prefetch=1,
            grid=(group,),
            in_specs=[
                pl.BlockSpec((1, 8, seq_len), by_place),
                pl.BlockSpec((1, seq_len, model_dim), by_place),
            ],
            out_specs=pl.BlockSpec((1, aligned_rows, model_dim), by_place),
        ),
        out_shape=jax.ShapeDtypeStruct((group, aligned_rows, model_dim), BF16),
        compiler_params=pltpu.CompilerParams(vmem_limit_bytes=VMEM_LIMIT),
        cost_estimate=pl.CostEstimate(
            flops=2 * group * aligned_rows * seq_len * model_dim,
            bytes_accessed=2 * group * (aligned_rows + seq_len) * model_dim,
            transcendentals=NONE,
        ),
        name="select",
    )(me, codes, u_all)


def expert_kernel(
    segment_sizes, me_ref, count_ref, x_in, gate_ref, up_ref, down_ref, x_out,
    buf, blocks_ref, offset_ref, total_ref, in_sem, out_sem,
):
    step = pl.program_id(0)
    steps = pl.num_programs(0)
    places = x_in.shape[0]

    def each_segment(expert, slot, fn):
        def per_place(place, filled):
            n = blocks_ref[place, expert]
            first = offset_ref[place, expert]
            for size in segment_sizes:

                @pl.when(n // size % 2 == 1)
                def _():
                    done = n // (2 * size) * (2 * size)
                    rows = pl.ds(pl.multiple_of(first + done * BLOCK, BLOCK), size * BLOCK)
                    held = pl.ds(pl.multiple_of((filled + done) * BLOCK, BLOCK), size * BLOCK)
                    fn(place, rows, buf.at[slot, held], slot)

            return filled + n

        lax.fori_loop(0, places, per_place, jnp.int32(0))

    def fetch(place, rows, held, slot):
        pltpu.make_async_copy(x_in.at[place, rows], held, in_sem.at[slot]).start()

    def put(place, rows, held, slot):
        pltpu.make_async_copy(held, x_out.at[place, rows], out_sem.at[slot]).start()

    def fetched(n, slot):
        rows = pl.ds(0, n * BLOCK)
        pltpu.make_async_copy(x_in.at[0, rows], buf.at[slot, rows], in_sem.at[slot]).wait()

    def gone(n, slot):
        rows = pl.ds(0, n * BLOCK)
        pltpu.make_async_copy(buf.at[slot, rows], x_out.at[0, rows], out_sem.at[slot]).wait()

    def over(expert, fn):
        each_segment(expert, lax.rem(expert, 3), fn)

    def wait_all(expert, fn):
        slot = lax.rem(expert, 3)
        n = total_ref[expert]

        def most(i, _):
            fn(16, slot)
            return 0

        repeat(n // 16, most)
        for size in (8, 4, 2, 1):

            @pl.when(n // size % 2 == 1)
            def _():
                fn(size, slot)

        return n

    @pl.when(step == 0)
    def _():
        def plan(place, _):
            def one(e, filled):
                n = (count_ref[place, me_ref[0] * steps + e] + (BLOCK - 1)) // BLOCK
                blocks_ref[place, e] = n
                offset_ref[place, e] = filled * BLOCK
                total_ref[e] = jnp.where(place == 0, 0, total_ref[e]) + n
                return filled + n

            lax.fori_loop(0, steps, one, jnp.int32(0))
            return 0

        repeat(places, plan)
        over(step, fetch)

    @pl.when(step >= 2)
    def _():
        wait_all(step - 2, gone)

    @pl.when(step + 1 < steps)
    def _():
        over(step + 1, fetch)

    filled = wait_all(step, fetched)
    slot = lax.rem(step, 3)

    def tile(i, _):
        rows = pl.ds(pl.multiple_of(i * TILE, TILE), TILE)
        x = buf[slot, rows]
        gate = jnp.dot(x, gate_ref[0], preferred_element_type=F32)
        up = jnp.dot(x, up_ref[0], preferred_element_type=F32)
        hidden = (gate * jax.nn.sigmoid(gate) * up).astype(BF16)
        buf[slot, rows] = jnp.dot(hidden, down_ref[0], preferred_element_type=F32).astype(BF16)
        return 0

    repeat((filled * BLOCK + TILE - 1) // TILE, tile)
    over(step, put)

    @pl.when(step + 1 == steps)
    def _():
        wait_all(step - 1, gone)
        wait_all(step, gone)


def expert_ffn(me, counts, x, w_gate, w_up, w_down, capacity):
    places, aligned_rows, model_dim = x.shape
    experts, _, hidden_dim = w_gate.shape
    held = -(-places * capacity // TILE) * TILE
    most = -(-capacity // BLOCK)
    segment_sizes = [1 << i for i in reversed(range(most.bit_length()))]
    weight_in = pl.BlockSpec((1, model_dim, hidden_dim), by_place)
    return pl.pallas_call(
        functools.partial(expert_kernel, segment_sizes),
        grid_spec=pltpu.PrefetchScalarGridSpec(
            num_scalar_prefetch=2,
            grid=(experts,),
            in_specs=[
                pl.BlockSpec(memory_space=pl.ANY),
                weight_in,
                weight_in,
                pl.BlockSpec((1, hidden_dim, model_dim), by_place),
            ],
            out_specs=pl.BlockSpec(memory_space=pl.ANY),
            scratch_shapes=[
                pltpu.VMEM((3, held, model_dim), BF16),
                pltpu.SMEM((places, experts), I32),
                pltpu.SMEM((places, experts), I32),
                pltpu.SMEM((experts,), I32),
                pltpu.SemaphoreType.DMA((3,)),
                pltpu.SemaphoreType.DMA((3,)),
            ],
        ),
        out_shape=jax.ShapeDtypeStruct(x.shape, BF16),
        input_output_aliases={2: 0},
        compiler_params=pltpu.CompilerParams(vmem_limit_bytes=VMEM_LIMIT),
        cost_estimate=pl.CostEstimate(
            flops=6 * 3072 * model_dim * hidden_dim,
            bytes_accessed=6 * experts * model_dim * hidden_dim,
            transcendentals=NONE,
        ),
        name="experts",
    )(me, counts, x, w_gate, w_up, w_down)


def pack_kernel(local_experts, me_ref, count_ref, x_ref, out_ref):
    rows_out, aligned_rows = out_ref.shape[1], x_ref.shape[1]
    place = pl.program_id(0)
    chunk = rows_out if rows_out <= 512 else 256
    for first in range(0, rows_out, chunk):
        row = row_ids((chunk, 1)) + first
        source = jnp.full((chunk, 1), -1, I32)
        off, aligned_off = jnp.int32(0), jnp.int32(0)
        for e in range(local_experts):
            n = count_ref[place, me_ref[0] * local_experts + e]
            inside = (row >= off) & (row < off + n)
            source = jnp.where(inside, row + (aligned_off - off), source)
            off = off + n
            aligned_off = aligned_off + (n + (BLOCK - 1)) // BLOCK * BLOCK
        col = col_ids((chunk, aligned_rows))
        pick = jnp.where(col == source, 1.0, 0.0).astype(BF16)
        out_ref[0, first : first + chunk] = jnp.dot(pick, x_ref[0], preferred_element_type=F32).astype(BF16)


def pack_rows(me, counts, x, local_experts, aligned_rows, rows_out):
    places, _, model_dim = x.shape
    return pl.pallas_call(
        functools.partial(pack_kernel, local_experts),
        grid_spec=pltpu.PrefetchScalarGridSpec(
            num_scalar_prefetch=2,
            grid=(places,),
            in_specs=[pl.BlockSpec((1, aligned_rows, model_dim), by_place)],
            out_specs=pl.BlockSpec((1, rows_out, model_dim), by_place),
        ),
        out_shape=jax.ShapeDtypeStruct((places, rows_out, model_dim), BF16),
        compiler_params=pltpu.CompilerParams(vmem_limit_bytes=VMEM_LIMIT),
        cost_estimate=pl.CostEstimate(
            flops=2 * places * aligned_rows * rows_out * model_dim,
            bytes_accessed=2 * places * (aligned_rows + rows_out) * model_dim,
            transcendentals=NONE,
        ),
        name="pack",
    )(me, counts, x)


def combine_kernel(top_k, code_ref, gates_ref, recv_ref, h_ref, out_ref, acc_ref):
    step = pl.program_id(0)
    rows = recv_ref.shape[0]

    @pl.when(step == 0)
    def _():
        acc_ref[...] = h_ref[...].astype(F32)

    code = code_ref[...]
    gates = gates_ref[...]
    col = col_ids((code.shape[0], rows)) + step * rows
    mix = jnp.zeros(col.shape, F32)
    for j in range(top_k):
        mix = jnp.where(col == code[:, j : j + 1], gates[:, j : j + 1], mix)
    acc_ref[...] += jnp.dot(mix.astype(BF16), recv_ref[...], preferred_element_type=F32)

    @pl.when(step == pl.num_programs(0) - 1)
    def _():
        out_ref[...] = acc_ref[...].astype(BF16)


def combine(residual, recv, code, gates):
    seq_len, model_dim = residual.shape
    group, rows, _ = recv.shape
    top_k = gates.shape[1]
    column = jnp.where(code >= 0, code // BASE * rows + code % BASE, -1)
    gates_f = jnp.pad(gates.astype(F32), ((0, 0), (0, 8 - top_k)))
    rows_step = 256
    whole = lambda r, c: pl.BlockSpec((r, c), at_origin)
    return pl.pallas_call(
        functools.partial(combine_kernel, top_k),
        grid=(group * rows // rows_step,),
        in_specs=[
            whole(seq_len, 8),
            whole(seq_len, 8),
            pl.BlockSpec((rows_step, model_dim), lambda i: (i, 0)),
            whole(seq_len, model_dim),
        ],
        out_specs=whole(seq_len, model_dim),
        out_shape=jax.ShapeDtypeStruct((seq_len, model_dim), BF16),
        scratch_shapes=[pltpu.VMEM((seq_len, model_dim), F32)],
        compiler_params=pltpu.CompilerParams(vmem_limit_bytes=VMEM_LIMIT),
        cost_estimate=pl.CostEstimate(
            flops=2 * seq_len * group * rows * model_dim,
            bytes_accessed=2 * (group * rows + 2 * seq_len) * model_dim,
            transcendentals=NONE,
        ),
        name="combine",
    )(column, gates_f, recv.reshape(group * rows, model_dim), residual)


def back_kernel(
    group, top_k, packed_ref, got_ref, codes_ref, gates_ref, ha_ref, hb_ref, outa_ref, outb_ref,
    recv, held, acc, own_sem, held_sem, send_sem, recv_sem,
):
    seq_len, model_dim = ha_ref.shape
    rows = recv.shape[1]
    chips = group // 2
    me = lax.axis_index("ep")
    chip, core = me // 2, lax.rem(me, 2)

    def device_at(place):
        pair = place // 2
        away = pair + pair // 2 - 2 * (pair // 3)
        return lax.rem(chip + away, chips) * 2 + lax.rem(core + place, 2)

    def copy(place):
        seen = (0, 1, 4, 5, 2, 3, 6, 7)[place]
        to = device_at(place)
        return pltpu.make_async_remote_copy(
            src_ref=packed_ref.at[to], dst_ref=recv.at[me], send_sem=send_sem.at[place], recv_sem=recv_sem.at[seen],
            device_id={"ep": to}, device_id_type=pl.DeviceIdType.MESH,
        )

    def hold(source, slot):
        return pltpu.make_async_copy(got_ref.at[source], held.at[slot], held_sem.at[slot])

    barrier = pltpu.get_barrier_semaphore()
    for d in range(1, group):
        pl.semaphore_signal(barrier, device_id={"ep": lax.rem(me + d, group)}, device_id_type=pl.DeviceIdType.MESH)
    hold(0, 0).start()
    own = pltpu.make_async_copy(packed_ref.at[me], recv.at[me], own_sem)
    own.start()
    pl.semaphore_wait(barrier, group - 1)
    for place in (1, 2, 4, 3, 5, 6, 7):
        copy(place).start()

    def mix_of(batch, source):
        code = codes_ref[batch] - source * BASE
        gates = gates_ref[batch]
        col = col_ids((seq_len, rows))
        mix = jnp.zeros((seq_len, rows), F32)
        for j in range(top_k):
            mix = jnp.where(col == code[:, j : j + 1], gates[:, j : j + 1], mix)
        return mix.astype(BF16)

    def begin(h_ref):
        for piece in pieces(seq_len):
            acc[piece] = h_ref[piece].astype(F32)

    def finish(out_ref):
        for piece in pieces(seq_len):
            out_ref[piece] = acc[piece].astype(BF16)

    begin(ha_ref)

    def add_a(source, _):
        slot = lax.rem(source, 2)

        @pl.when(source + 1 < group)
        def _():
            hold(source + 1, 1 - slot).start()

        mix = mix_of(0, source)
        hold(source, slot).wait()
        acc[...] += jnp.dot(mix, held[slot], preferred_element_type=F32)
        return 0

    repeat(group, add_a)
    finish(outa_ref)
    begin(hb_ref)

    def add_b(place, _):
        source = device_at(place)
        mix = mix_of(1, source)

        @pl.when(place == 0)
        def _():
            own.wait()

        @pl.when(place > 0)
        def _():
            pltpu.make_async_remote_copy(
                src_ref=packed_ref.at[source], dst_ref=recv.at[source], send_sem=send_sem.at[place],
                recv_sem=recv_sem.at[place], device_id={"ep": source}, device_id_type=pl.DeviceIdType.MESH,
            ).wait_recv()

        acc[...] += jnp.dot(mix, recv[source], preferred_element_type=F32)
        return 0

    repeat(group, add_b)
    finish(outb_ref)
    for place in range(1, group):
        copy(place).wait_send()


def return_and_combine(packed_b, back_a, h_a, h_b, codes, gates, group):
    seq_len, model_dim = h_a.shape
    rows = packed_b.shape[1]
    top_k = gates.shape[2]
    gates_f = jnp.pad(gates.astype(F32), ((0, 0), (0, 0), (0, 8 - top_k)))
    vmem = pl.BlockSpec(memory_space=pltpu.VMEM)
    anywhere = pl.BlockSpec(memory_space=pl.ANY)
    dma = pltpu.SemaphoreType.DMA
    pair = dma((2,))
    return pl.pallas_call(
        functools.partial(back_kernel, group, top_k),
        in_specs=[anywhere, anywhere, vmem, vmem, vmem, vmem],
        out_specs=[vmem, vmem],
        out_shape=[jax.ShapeDtypeStruct((seq_len, model_dim), BF16)] * 2,
        scratch_shapes=[
            pltpu.VMEM((group, rows, model_dim), BF16),
            pltpu.VMEM((2, rows, model_dim), BF16),
            pltpu.VMEM((seq_len, model_dim), F32),
            dma,
            pair,
            dma((group,)),
            dma((group,)),
        ],
        compiler_params=pltpu.CompilerParams(vmem_limit_bytes=VMEM_LIMIT, collective_id=1, has_side_effects=True),
        cost_estimate=pl.CostEstimate(
            flops=4 * seq_len * group * rows * model_dim,
            bytes_accessed=2 * (4 * group * rows + 4 * seq_len) * model_dim,
            transcendentals=NONE,
        ),
        name="back",
    )(packed_b, back_a, codes, gates_f, h_a, h_b)


def emit_kernel(a_ref, b_ref, outa_ref, outb_ref):
    outa_ref[...] = a_ref[...]
    outb_ref[...] = b_ref[...]


def emit(a, b):
    seq_len, model_dim = a.shape
    block = pl.BlockSpec((seq_len // 4, model_dim), lambda i: (i, 0))
    return pl.pallas_call(
        emit_kernel,
        grid=(4,),
        in_specs=[block, block],
        out_specs=[block, block],
        out_shape=[jax.ShapeDtypeStruct(a.shape, BF16)] * 2,
        compiler_params=pltpu.CompilerParams(vmem_limit_bytes=VMEM_LIMIT // 2),
        cost_estimate=SMALL,
        name="emit",
    )(a, b)


def capacity_of(seq_len, top_k, experts_total):
    return 8 * max(1, (seq_len * top_k) // (4 * experts_total))


def solution(mesh):
    group = mesh.shape["ep"]
    row_spec = P(("dp", "ep"), None)
    full_spec = P(None, None, None)
    gain_spec = P(None)
    expert_spec = P("ep", None, None)
    in_specs = (row_spec,) * 8 + (gain_spec, full_spec, full_spec, full_spec, full_spec, gain_spec) + (expert_spec,) * 3

    def device_fn(
        tokens_a, experts_a, slots_a, gates_a, tokens_b, experts_b, slots_b, gates_b,
        attn_gain, w_query, w_key, w_value, w_out, moe_gain, w_gate, w_up, w_down,
    ):
        seq_len, model_dim = tokens_a.shape
        local_experts = w_gate.shape[0]
        capacity = capacity_of(seq_len, experts_a.shape[1], local_experts * group)
        full_rows = local_experts * capacity
        me = lax.axis_index("ep").astype(I32)

        top_k = experts_a.shape[1]
        me1 = me.reshape(1)
        table, exact = route(jnp.stack([experts_a, experts_b]), jnp.stack([slots_a, slots_b]), local_experts, group)
        h_a, h_b, u_all_a, u_b, tables, x_a = front(
            tokens_a, tokens_b, w_query, w_key, w_value, w_out, attn_gain, moe_gain, table, group, top_k, full_rows
        )
        counts = tables[:, :, COUNT_ROW, : local_experts * group].transpose(1, 0, 2)
        codes = tables.transpose(1, 0, 2, 3)
        largest = jnp.max(tables[:, :, MOST_ROW, 0])
        packed_rows = 352

        def packed_outputs(x, counts_b, aligned_rows, rows_out):
            o = expert_ffn(me1, counts_b, x, w_gate, w_up, w_down, capacity)
            return pack_rows(me1, counts_b, o, local_experts, aligned_rows, rows_out)

        def usual(operands):
            x_a, u_all_a, u_b, h_a, h_b, codes, counts, exact = operands
            aligned_rows = min(full_rows, -(-(packed_rows + local_experts * (BLOCK - 1)) // 160) * 160)
            u_all_b = lax.all_gather(u_b, "ep", axis=0, tiled=False)
            packed_a = packed_outputs(x_a, counts[0], aligned_rows, packed_rows)
            back_a = lax.all_to_all(packed_a, "ep", 0, 0, tiled=True)
            x_b = select_rows(me1, codes[1], u_all_b, aligned_rows, top_k)
            packed_b = packed_outputs(x_b, counts[1], aligned_rows, packed_rows)
            gates = jnp.stack([gates_a, gates_b])
            return tuple(emit(*return_and_combine(packed_b, back_a, h_a, h_b, exact, gates, group)))

        def fullest(operands):
            x_a, u_all_a, u_b, h_a, h_b, codes, counts, exact = operands
            u_all_b = lax.all_gather(u_b, "ep", axis=0, tiled=False)

            def one(batch):
                u_all, h, codes_b, counts_b, exact_b, gates_b = batch
                x = select_rows(me1, codes_b, u_all, full_rows, top_k)
                back = lax.all_to_all(packed_outputs(x, counts_b, full_rows, full_rows), "ep", 0, 0, tiled=True)
                return combine(h, back, exact_b, gates_b)

            both = lax.map(
                one,
                (jnp.stack([u_all_a, u_all_b]), jnp.stack([h_a, h_b]), codes, counts, exact, jnp.stack([gates_a, gates_b])),
            )
            return both[0], both[1]

        operands = (x_a, u_all_a, u_b, h_a, h_b, codes, counts, exact)
        return lax.cond(largest <= packed_rows, usual, fullest, operands)

    return jax.shard_map(device_fn, mesh=mesh, in_specs=in_specs, out_specs=(row_spec, row_spec), check_vma=False)
```
